32 devices in a mesh: group: 2 (over y), temp: 4 (over x, core), gz: 4 (over z).
Axes of the slice: x: 2, y: 2, z: 4, core: 2. Of those that a mesh axis runs over, the one named last changes fastest.
Arguments:
- spin_state: float32 [16, 3, 16, 128, 128], P(('group', 'temp'), None, 'gz'), parts along dimension 0, may hold values from -1 to 1, as said below
- couplings: float32 [3, 32, 128, 128], P(None, ('group', 'gz')), parts along dimension 1, may hold values from -12 to 12
- inverse_temps: float32 [16], P(('group', 'temp')), parts along dimension 0, may hold values from 0.3 to 3
- colour_order: int32 [16], P(('group', 'temp')), parts along dimension 0, may hold values 0 or 1
- heat_level: float32 [16, 16, 128, 128], P(('group', 'temp'), 'gz'), parts along dimension 0, may hold values from 0.001 to 0.999
- heat_height: float32 [16, 16, 128, 128], P(('group', 'temp'), 'gz'), parts along dimension 0, may hold values from -1 to 1
- heat_angle: float32 [16, 16, 128, 128], P(('group', 'temp'), 'gz'), parts along dimension 0, may hold values from -3.140625 to 3.140625
- swap_bits: int32 [16], P(('group', 'temp')), parts along dimension 0, may hold values 0 or 1
Outputs:
- spin_final: float32 [16, 3, 16, 128, 128], P(('group', 'temp'), None, 'gz'), parts along dimension 0
- energies: float32 [16], P(('group', 'temp')), parts along dimension 0
The draws below stay inside these ranges and needn't reach their ends.
There are 2 independent parts, one for each index of `group`. The reference program is written for one: setup_inputs(seed, part) draws one part's arguments, and reference() takes and returns one part's arrays. A program takes and returns all parts, laid end to end along the dimension named above; each array names one. Nothing has to cross between parts.
Inputs may be any that keep to these rules, and one draw needn't show every extreme that they name: `spin_state`: every site's three components form a vector of unit length.
All inputs are finite; a program needn't handle non-finite values. No bound on the sum of `colour_order` or of `swap_bits` on one device may be relied on, other than what follows from the above.
Results may differ from the reference program's by a relative error of at most 0.0003.
Values sent between devices are 32-bit elements; how exact they have to be, the bound alone decides.
A program may use at most 64 MiB of HBM per device.

```python
import math
import jax
import jax.numpy as jnp
from jax import lax

LX = 128
LY = 128
OR_SWEEPS = 2
REPLICAS = 8
NZ = 16


def draw_spin_state(key, part):
    first_key, second_key = jax.random.split(jax.random.fold_in(key, 11))
    array_shape = (REPLICAS, NZ, LY, LX)
    height = jax.random.uniform(first_key, array_shape, jnp.float32, -1.0, 1.0)
    azimuth = jax.random.uniform(second_key, array_shape, jnp.float32, -math.pi, math.pi)
    side = jnp.sqrt(jnp.maximum(1.0 - height * height, 0.0))
    return jnp.stack([side * jnp.cos(azimuth), side * jnp.sin(azimuth), height], axis=1)


def draw_couplings(key, part):
    first_key = jax.random.fold_in(key, 23)
    array_shape = (3, NZ, LY, LX)
    position = jnp.arange(NZ, dtype=jnp.float32) / max(NZ - 1, 1)
    values = jnp.clip(jax.random.normal(first_key, array_shape, jnp.float32), -4.0, 4.0)
    factor = 1.0 + 2.0 * position
    return values * factor[None, :, None, None]


def place_ends(array, rng, smallest, largest):
    longest = array.shape.index(max(array.shape))
    spots = []
    for shift in (0, 1):
        where = [jax.random.randint(jax.random.fold_in(rng, axis), (), 0, length) for axis, length in enumerate(array.shape)]
        where[longest] = (where[longest] + shift) % array.shape[longest]
        spots.append(tuple(where))
    return array.at[spots[0]].set(smallest).at[spots[1]].set(largest)


def steps_of(rng, dims, shards, low, largest):
    level = 1.0
    for dim, blocks in shards:
        draws = jax.random.uniform(jax.random.fold_in(jax.random.fold_in(rng, 6), dim), (blocks,), jnp.float32, low / len(shards), largest / len(shards))
        level = level * jnp.repeat(jnp.exp(draws), dims[dim] // blocks).reshape((-1,) + (1,) * (len(dims) - 1 - dim))
    return level


def setup_inputs(seed: int = 0, part: int = 0) -> dict:
    streams_of = jax.random.split(jax.random.key(seed), 9)
    part_splits = jax.random.split(jax.random.fold_in(streams_of[8], part), 9)
    return {
        "spin_state": draw_spin_state(jax.random.fold_in(jax.random.fold_in(streams_of[8], part), 71), part),
        "couplings": draw_couplings(jax.random.fold_in(jax.random.fold_in(streams_of[8], part), 71), part),
        "inverse_temps": jnp.clip(jnp.exp(math.log(3.0) - 2.3025851 * jax.random.uniform(part_splits[2], (REPLICAS,), jnp.float32) ** steps_of(part_splits[2], (REPLICAS,), ((0, 4),), -0.2, 0.2)), 0.3, 3.0),
        "colour_order": place_ends((jax.random.randint(part_splits[3], (REPLICAS,), 0, 2) < 1).astype(jnp.int32), jax.random.fold_in(part_splits[3], 1), 0, 1),
        "heat_level": jnp.clip(0.001 + 0.998 * jax.random.uniform(part_splits[4], (REPLICAS, NZ, LY, LX), jnp.float32) ** steps_of(part_splits[4], (REPLICAS, NZ, LY, LX), ((0, 4), (1, 4)), -0.2, 0.2), 0.001, 0.999),
        "heat_height": jnp.clip(jax.random.uniform(part_splits[5], (REPLICAS, NZ, LY, LX), jnp.float32, -1.0, 1.0) * steps_of(part_splits[5], (REPLICAS, NZ, LY, LX), ((0, 4), (1, 4)), -0.4, 0.0), -1.0, 1.0),
        "heat_angle": jnp.clip(jax.random.uniform(part_splits[6], (REPLICAS, NZ, LY, LX), jnp.float32, -3.140625, 3.140625), -3.140625, 3.140625),
        "swap_bits": place_ends((jax.random.randint(part_splits[7], (REPLICAS,), 0, 4) < 3).astype(jnp.int32), jax.random.fold_in(part_splits[7], 1), 0, 1),
    }


def neighbour_sum(current, bonds):
    east_bond, north_bond, upper_bond = (bonds[0], bonds[1], bonds[2])
    summed = east_bond * jnp.roll(current, -1, 3) + jnp.roll(east_bond, 1, 2) * jnp.roll(current, 1, 3)
    summed = summed + north_bond * jnp.roll(current, -1, 2) + jnp.roll(north_bond, 1, 1) * jnp.roll(current, 1, 2)
    summed = summed + upper_bond * jnp.roll(current, -1, 1) + jnp.roll(upper_bond, 1, 0) * jnp.roll(current, 1, 1)
    return summed

def reflect(current, pulled, component_axis):
    projection = lax.optimization_barrier(jnp.sum(current * pulled, axis=component_axis, keepdims=True))
    square = lax.optimization_barrier(jnp.sum(pulled * pulled, axis=component_axis, keepdims=True))
    return 2.0 * projection / jnp.maximum(square, 0.01) * pulled - current

def heat_bath(pulled, beta_value, uniform_level, cosine_draw, angle_draw, component_axis):
    square = lax.optimization_barrier(jnp.sum(pulled * pulled, axis=component_axis, keepdims=True))
    strength = jnp.sqrt(jnp.maximum(square, 0.01))
    unit_axis = pulled / strength
    reach = beta_value * strength
    cosine = 1.0 + jnp.log1p(uniform_level * jnp.expm1(-2.0 * reach)) / reach
    side = jnp.sqrt(jnp.maximum(1.0 - cosine_draw * cosine_draw, 0.0))
    proposal = jnp.concatenate([side * jnp.cos(angle_draw), side * jnp.sin(angle_draw), cosine_draw], axis=component_axis)
    along_axis = lax.optimization_barrier(jnp.sum(proposal * unit_axis, axis=component_axis, keepdims=True))
    tangent = proposal - along_axis * unit_axis
    tangent = tangent / jnp.sqrt(jnp.maximum(lax.optimization_barrier(jnp.sum(tangent * tangent, axis=component_axis, keepdims=True)), 0.0001))
    return cosine * unit_axis + jnp.sqrt(jnp.maximum(1.0 - cosine * cosine, 0.0)) * tangent

def pair_swap(stacked, decisions):
    flipped = stacked[:, ::-1]
    taking = (decisions != 0).reshape((-1,) + (1,) * (stacked.ndim - 1))
    return jnp.where(taking, flipped, stacked)

def reference(spin_state, couplings, inverse_temps, colour_order, heat_level, heat_height, heat_angle, swap_bits):
    plane_index = jnp.arange(NZ, dtype=jnp.int32)
    row_index = jnp.arange(LY, dtype=jnp.int32)
    column_index = jnp.arange(LX, dtype=jnp.int32)
    site_sum = plane_index[:, None, None] + row_index[None, :, None] + column_index[None, None, :]

    def one_replica(packed):
        current, beta_value, start_colour, uniform_level, cosine_draw, angle_draw = packed
        parity = (site_sum + start_colour) % 2
        colours = ((parity == 0)[None], (parity == 1)[None])
        for sweep_index in range(OR_SWEEPS):
            for chosen in colours:
                pulled = neighbour_sum(current, couplings)
                current = jnp.where(chosen, reflect(current, pulled, 0), current)
        for chosen in colours:
            pulled = neighbour_sum(current, couplings)
            renewed = heat_bath(pulled, beta_value, uniform_level[None], cosine_draw[None], angle_draw[None], 0)
            current = jnp.where(chosen, renewed, current)
        bond_sum = couplings[0] * jnp.roll(current, -1, 3) + couplings[1] * jnp.roll(current, -1, 2) + couplings[2] * jnp.roll(current, -1, 1)
        energy = -jnp.sum(current * bond_sum) / (LX * LY * NZ)
        return (current, energy)
    swept, energy_all = lax.map(one_replica, (spin_state, inverse_temps, colour_order, heat_level, heat_height, heat_angle))
    count = REPLICAS
    tail_shape = swept.shape[1:]
    swept = pair_swap(swept.reshape((count // 2, 2) + tail_shape), swap_bits[0::2]).reshape(swept.shape)
    energy_all = pair_swap(energy_all.reshape((count // 2, 2)), swap_bits[0::2]).reshape((count,))
    middle = pair_swap(swept[1:count - 1].reshape(((count - 2) // 2, 2) + tail_shape), swap_bits[1:count - 1:2])
    swept = jnp.concatenate([swept[:1], middle.reshape((count - 2,) + tail_shape), swept[count - 1:]], axis=0)
    middle_energy = pair_swap(energy_all[1:count - 1].reshape(((count - 2) // 2, 2)), swap_bits[1:count - 1:2])
    energy_all = jnp.concatenate([energy_all[:1], middle_energy.reshape((count - 2,)), energy_all[count - 1:]], axis=0)
    return (swept, energy_all)
```

```python
import functools
import math

import jax
import jax.numpy as jnp
from jax import lax
from jax.experimental import pallas as pl
from jax.experimental.pallas import tpu as pltpu
from jax.sharding import PartitionSpec as P

OR_SWEEPS = 2
HALVES = 2 * OR_SWEEPS + 2
PAD = 8
MESH = pl.DeviceIdType.MESH
SIN_TERMS = [(-1.0) ** i / math.factorial(2 * i + 1) for i in range(8)]
COS_TERMS = [(-1.0) ** i / math.factorial(2 * i) for i in range(9)]


def horner(terms, value):
    total = jnp.full_like(value, terms[-1])
    for term in terms[-2::-1]:
        total = total * value + term
    return total


def cos_sin(angle):
    half = 0.5 * angle
    square = half * half
    sine = half * horner(SIN_TERMS, square)
    cosine = horner(COS_TERMS, square)
    return 1.0 - 2.0 * sine * sine, 2.0 * sine * cosine


def dot3(a, b):
    return a[0] * b[0] + a[1] * b[1] + a[2] * b[2]


def reflect(current, pulled):
    factor = 2.0 * dot3(current, pulled) / jnp.maximum(dot3(pulled, pulled), 0.01)
    return [factor * p - s for p, s in zip(pulled, current)]


def heat_bath(pulled, beta, level, trial):
    strength = jnp.sqrt(jnp.maximum(dot3(pulled, pulled), 0.01))
    inverse = 1.0 / strength
    axis = [p * inverse for p in pulled]
    reach = beta * strength
    shrink = -jnp.tanh(reach) * (jnp.exp(-2.0 * reach) + 1.0)
    cosine = 1.0 + jnp.log1p(level * shrink) / reach
    along = dot3(trial, axis)
    tangent = [t - along * a for t, a in zip(trial, axis)]
    scale = jnp.sqrt(jnp.maximum(1.0 - cosine * cosine, 0.0)) * (
        1.0 / jnp.sqrt(jnp.maximum(dot3(tangent, tangent), 0.0001))
    )
    return [cosine * a + scale * t for a, t in zip(axis, tangent)]


def kernel(
    dims,
    spin_hbm,
    coup_hbm,
    beta_ref,
    order_ref,
    level_hbm,
    height_hbm,
    angle_hbm,
    bits_ref,
    out_ref,
    eout_ref,
    spin_in,
    coup_in,
    level_in,
    height_in,
    angle_in,
    below_bond,
    sp,
    xo,
    xr,
    yi,
    yo,
    zu,
    zd,
    lv,
    ut,
    eacc,
    ebuf,
    tsend,
    trecv,
    rbuf,
    in_sem,
    bond_sem,
    hsend,
    hrecv,
    esend,
    erecv,
    tssem,
    trsem,
    xsend,
    xrecv,
):
    count, planes, rows, width, n, m = dims
    k = rows // 2
    chunk = 32 if k % 32 == 0 else 8
    g = lax.axis_index("gz")
    t = lax.axis_index("temp")
    up, down = lax.rem(g + 1, n), lax.rem(g + n - 1, n)
    has_below, has_above = t > 0, t < m - 1

    loads = [
        pltpu.make_async_copy(src, dst, in_sem.at[i])
        for i, (src, dst) in enumerate(
            (
                (spin_hbm, spin_in),
                (coup_hbm, coup_in),
                (level_hbm, level_in),
                (height_hbm, height_in),
                (angle_hbm, angle_in),
            )
        )
    ]
    for load in loads:
        load.start()

    barrier = pltpu.get_barrier_semaphore()
    for d in range(1, n):
        pl.semaphore_signal(
            barrier, inc=1, device_id={"gz": lax.rem(g + d, n)}, device_id_type=MESH
        )

    @pl.when(has_below)
    def _():
        pl.semaphore_signal(barrier, inc=1, device_id={"temp": t - 1}, device_id_type=MESH)

    @pl.when(has_above)
    def _():
        pl.semaphore_signal(barrier, inc=1, device_id={"temp": t + 1}, device_id_type=MESH)

    pl.semaphore_wait(barrier, n - 1 + has_below.astype(jnp.int32) + has_above.astype(jnp.int32))

    def parity(r, z, size):
        lane = lax.broadcasted_iota(jnp.int32, (size, width), 1)
        return ((lane + (g * planes + z + order_ref[r])) & 1) != 0

    def halves(ref, index, start, size):
        even = ref[index + (pl.ds(2 * start, size, stride=2), slice(None))]
        odd = ref[index + (pl.ds(2 * start + 1, size, stride=2), slice(None))]
        return even, odd

    def put_spin(c, r, d, z, start, value):
        size = value.shape[0]
        sp[c, r, d, z + 1, pl.ds(PAD + start, size), :] = value
        if start == 0:
            sp[c, r, d, z + 1, pl.ds(PAD + k, 1), :] = value[0:1]
        if start + size == k:
            sp[c, r, d, z + 1, pl.ds(PAD - 1, 1), :] = value[size - 1 : size]

    def pack_spin(r, z):
        e = parity(r, z, k)
        for d in range(3):
            even, odd = halves(spin_in, (r, d, z), 0, k)
            put_spin(0, r, d, z, 0, jnp.where(e, odd, even))
            put_spin(1, r, d, z, 0, jnp.where(e, even, odd))

    def halo(x, r, side):
        c = 1 - x % 2
        source, target = (1, planes + 1) if side == 0 else (planes, 0)
        return pltpu.make_async_remote_copy(
            src_ref=sp.at[c, r, :, source, pl.ds(PAD, k), :],
            dst_ref=sp.at[c, r, :, target, pl.ds(PAD, k), :],
            send_sem=hsend.at[x, r, side],
            recv_sem=hrecv.at[x, r, side],
            device_id={"gz": down if side == 0 else up},
            device_id_type=MESH,
        )

    def edges(r, action):
        def step(i, carry):
            action(r, i * (planes - 1))
            return carry

        lax.fori_loop(0, 2, step, 0)

    def inner(action):
        def step(i, carry):
            action(i // (planes - 2), 1 + i % (planes - 2))
            return carry

        if planes > 2:
            lax.fori_loop(0, count * (planes - 2), step, 0)

    loads[0].wait()
    for r in range(count):
        edges(r, pack_spin)
        for side in (0, 1):
            halo(0, r, side).start()
    loads[1].wait()
    bond = pltpu.make_async_remote_copy(
        src_ref=coup_in.at[2, planes - 1],
        dst_ref=below_bond,
        send_sem=bond_sem.at[0],
        recv_sem=bond_sem.at[1],
        device_id={"gz": up},
        device_id_type=MESH,
    )
    bond.start()
    inner(pack_spin)

    def pack_bonds(i, carry):
        r, z = i // planes, i % planes
        e = parity(r, z, k)
        even, odd = halves(coup_in, (0, z), 0, k)
        first, second = jnp.where(e, odd, even), jnp.where(e, even, odd)
        xo[0, r, z] = first
        xo[1, r, z] = second
        xr[0, r, z] = pltpu.roll(second, 1, 1)
        xr[1, r, z] = pltpu.roll(first, 1, 1)
        even, odd = halves(coup_in, (1, z), 0, k)
        before = pltpu.roll(odd, 1, 0)
        yi[r, z] = even
        yo[0, r, z] = jnp.where(e, odd, before)
        yo[1, r, z] = jnp.where(e, before, odd)
        even, odd = halves(coup_in, (2, z), 0, k)
        zu[0, r, z] = jnp.where(e, odd, even)
        zu[1, r, z] = jnp.where(e, even, odd)
        return carry

    def pack_lower(i, carry):
        r, z = i // (planes - 1), 1 + i % (planes - 1)
        e = parity(r, z, k)
        even, odd = halves(coup_in, (2, z - 1), 0, k)
        zd[0, r, z] = jnp.where(e, odd, even)
        zd[1, r, z] = jnp.where(e, even, odd)
        return carry

    lax.fori_loop(0, count * planes, pack_bonds, 0)
    lax.fori_loop(0, count * (planes - 1), pack_lower, 0)
    bond.wait()
    for r in range(count):
        e = parity(r, 0, k)
        even, odd = halves(below_bond, (), 0, k)
        zd[0, r, 0] = jnp.where(e, odd, even)
        zd[1, r, 0] = jnp.where(e, even, odd)

    def pull(c, r, z, start):
        o = 1 - c
        part = pl.ds(start, chunk)
        e = parity(r, z, chunk)
        bx, br, by = xo[c, r, z, part, :], xr[c, r, z, part, :], yi[r, z, part, :]
        bo, bu, bd = yo[c, r, z, part, :], zu[c, r, z, part, :], zd[c, r, z, part, :]
        pulled = []
        for d in range(3):
            mid = sp[o, r, d, z + 1, pl.ds(PAD + start, chunk), :]
            nxt = sp[o, r, d, z + 1, pl.ds(PAD + start + 1, chunk), :]
            prv = sp[o, r, d, z + 1, pl.ds(PAD + start - 1, chunk), :]
            outer = jnp.where(e, nxt, prv) if c == 0 else jnp.where(e, prv, nxt)
            total = bx * pltpu.roll(mid, width - 1, 1) + br * pltpu.roll(mid, 1, 1)
            total = total + by * mid + bo * outer
            total = total + bu * sp[o, r, d, z + 2, pl.ds(PAD + start, chunk), :]
            total = total + bd * sp[o, r, d, z, pl.ds(PAD + start, chunk), :]
            pulled.append(total)
        return pulled

    def relax(c, r, z):
        for start in range(0, k, chunk):
            pulled = pull(c, r, z, start)
            current = [sp[c, r, d, z + 1, pl.ds(PAD + start, chunk), :] for d in range(3)]
            for d, value in enumerate(reflect(current, pulled)):
                put_spin(c, r, d, z, start, value)

    def heat(c, r, z):
        for start in range(0, k, chunk):
            part = pl.ds(start, chunk)
            pulled = pull(c, r, z, start)
            trial = [ut[c, r, d, z, part, :] for d in range(3)]
            renewed = heat_bath(pulled, beta_ref[r], lv[c, r, z, part, :], trial)
            for d, value in enumerate(renewed):
                put_spin(c, r, d, z, start, value)
            if c == 1:
                terms = dot3(renewed, pulled)
                eacc[r] = eacc[r] + sum(terms[j : j + 8] for j in range(0, chunk, 8))

    def pack_heat(r):
        def step(z, carry):
            for start in range(0, k, chunk):
                part = pl.ds(start, chunk)
                e = parity(r, z, chunk)
                even, odd = halves(level_in, (r, z), start, chunk)
                lv[0, r, z, part, :] = jnp.where(e, odd, even)
                lv[1, r, z, part, :] = jnp.where(e, even, odd)
                angles = halves(angle_in, (r, z), start, chunk)
                heights = halves(height_in, (r, z), start, chunk)
                trials = []
                for angle, height in zip(angles, heights):
                    side = jnp.sqrt(jnp.maximum(1.0 - height * height, 0.0))
                    cosine, sine = cos_sin(angle)
                    trials.append((side * cosine, side * sine, height))
                for d in range(3):
                    ut[0, r, d, z, part, :] = jnp.where(e, trials[1][d], trials[0][d])
                    ut[1, r, d, z, part, :] = jnp.where(e, trials[0][d], trials[1][d])
            return carry

        lax.fori_loop(0, planes, step, 0)

    def take_halo(x, r):
        for side in (0, 1):
            halo(x, r, side).wait_recv()
            if x >= 1:
                halo(x - 1, r, side).wait_send()

    eacc[...] = jnp.zeros_like(eacc)
    for x in range(HALVES - 1):
        c = x % 2
        work = functools.partial(relax if x < 2 * OR_SWEEPS else heat, c)
        for r in range(count):
            take_halo(x, r)
            edges(r, work)
            for side in (0, 1):
                halo(x + 1, r, side).start()
        inner(work)
        if x == 0:
            for load in loads[2:]:
                load.wait()
        for r in range(count):
            if r % (2 * OR_SWEEPS) == x:
                pack_heat(r)

    def flag(j, size):
        return jnp.full((size, width), bits_ref[j], jnp.int32) != 0

    def unpack(z):
        for r in range(0, count, 2):
            taking = flag(r, k)
            masks = [parity(r + j, z, k) for j in (0, 1)]
            for d in range(3):
                both = []
                for j in (0, 1):
                    first = sp[0, r + j, d, z + 1, pl.ds(PAD, k), :]
                    second = sp[1, r + j, d, z + 1, pl.ds(PAD, k), :]
                    both.append(
                        (jnp.where(masks[j], second, first), jnp.where(masks[j], first, second))
                    )
                for row in (0, 1):
                    low, top = both[0][row], both[1][row]
                    place = pl.ds(row, k, stride=2)
                    out_ref[r, d, z, place, :] = jnp.where(taking, top, low)
                    out_ref[r + 1, d, z, place, :] = jnp.where(taking, low, top)

    def ship(z, side):
        return pltpu.make_async_remote_copy(
            src_ref=out_ref.at[count - 1 if side == 0 else 0, :, z],
            dst_ref=rbuf.at[side, :, z],
            send_sem=xsend.at[z, side],
            recv_sem=xrecv.at[z, side],
            device_id={"temp": t + 1 if side == 0 else t - 1},
            device_id_type=MESH,
        )

    def finish(plane_list):
        for z in plane_list:
            unpack(z)

            @pl.when(has_above)
            def _():
                ship(z, 0).start()

            @pl.when(has_below)
            def _():
                ship(z, 1).start()

    x = HALVES - 1
    work = functools.partial(heat, 1)
    inner(work)
    middle = list(range(1, planes - 1))
    outside = [0, planes - 1]
    finish(middle)
    for r in range(count):
        take_halo(x, r)
        edges(r, work)
    swaps = []
    for d in range(1, n):
        swaps.append(
            pltpu.make_async_remote_copy(
                src_ref=eacc,
                dst_ref=ebuf.at[d - 1],
                send_sem=esend.at[d - 1],
                recv_sem=erecv.at[d - 1],
                device_id={"gz": lax.rem(g + d, n)},
                device_id_type=MESH,
            )
        )
    for swap in swaps:
        swap.start()
    finish(outside)

    for swap in swaps:
        swap.wait()
    sites = float(width * rows * planes * n)
    energy = []
    for r in range(count):
        total = eacc[r]
        for d in range(n - 1):
            total = total + ebuf[d, r]
        summed = jnp.sum(jnp.sum(total, axis=0, keepdims=True), axis=1, keepdims=True)
        energy.append(jnp.broadcast_to(-summed / sites, (8, width)))
    for r in range(0, count, 2):
        taking = flag(r, 8)
        low, top = energy[r], energy[r + 1]
        energy[r], energy[r + 1] = jnp.where(taking, top, low), jnp.where(taking, low, top)
    tsend[0] = energy[count - 1]
    tsend[1] = jnp.full((8, width), bits_ref[count - 1], jnp.int32).astype(jnp.float32)
    tsend[2] = energy[0]

    def tell(side):
        part = pl.ds(0, 2) if side == 0 else pl.ds(2, 1)
        return pltpu.make_async_remote_copy(
            src_ref=tsend.at[part],
            dst_ref=trecv.at[part],
            send_sem=tssem.at[side],
            recv_sem=trsem.at[side],
            device_id={"temp": t + 1 if side == 0 else t - 1},
            device_id_type=MESH,
        )

    @pl.when(has_above)
    def _():
        tell(0).start()

    @pl.when(has_below)
    def _():
        tell(1).start()

    for r in range(1, count - 1, 2):
        taking = flag(r, 8)
        low, top = energy[r], energy[r + 1]
        energy[r], energy[r + 1] = jnp.where(taking, top, low), jnp.where(taking, low, top)
        wide = flag(r, rows)

        def exchange(i, carry):
            d, z = i // planes, i % planes
            a, b = out_ref[r, d, z], out_ref[r + 1, d, z]
            out_ref[r, d, z] = jnp.where(wide, b, a)
            out_ref[r + 1, d, z] = jnp.where(wide, a, b)
            return carry

        lax.fori_loop(0, 3 * planes, exchange, 0)

    for r in range(count):
        eout_ref[r] = jnp.max(energy[r])

    for r in range(count):
        for side in (0, 1):
            halo(x, r, side).wait_send()

    @pl.when(has_above)
    def _():
        tell(0).wait_send()
        tell(1).wait_recv()
        wide = flag(count - 1, rows)
        eout_ref[count - 1] = jnp.max(
            jnp.where(flag(count - 1, 8), trecv[2], energy[count - 1])
        )
        for z in middle + outside:
            ship(z, 0).wait_send()
            ship(z, 1).wait_recv()
            for d in range(3):
                out_ref[count - 1, d, z] = jnp.where(wide, rbuf[1, d, z], out_ref[count - 1, d, z])

    @pl.when(has_below)
    def _():
        tell(1).wait_send()
        tell(0).wait_recv()
        eout_ref[0] = jnp.max(jnp.where(trecv[1] > 0.5, trecv[0], energy[0]))
        wide = jnp.broadcast_to(trecv[1][0:1], (rows, width)) > 0.5
        for z in middle + outside:
            ship(z, 1).wait_send()
            ship(z, 0).wait_recv()
            for d in range(3):
                out_ref[0, d, z] = jnp.where(wide, rbuf[0, d, z], out_ref[0, d, z])


def on_device(n, m, spin, coup, beta, order, level, height, angle, bits):
    count, _, planes, rows, width = spin.shape
    k = rows // 2
    f32 = jnp.float32
    hbm = pl.BlockSpec(memory_space=pltpu.HBM)
    smem = pl.BlockSpec(memory_space=pltpu.SMEM)
    dma = pltpu.SemaphoreType.DMA
    bonds = pltpu.VMEM((2, count, planes, k, width), f32)
    return pl.pallas_call(
        functools.partial(kernel, (count, planes, rows, width, n, m)),
        out_shape=(
            jax.ShapeDtypeStruct(spin.shape, f32),
            jax.ShapeDtypeStruct((count,), f32),
        ),
        in_specs=[hbm, hbm, smem, smem, hbm, hbm, hbm, smem],
        out_specs=(pl.BlockSpec(memory_space=pltpu.VMEM), smem),
        scratch_shapes=[
            pltpu.VMEM(spin.shape, f32),
            pltpu.VMEM(coup.shape, f32),
            pltpu.VMEM(level.shape, f32),
            pltpu.VMEM(level.shape, f32),
            pltpu.VMEM(level.shape, f32),
            pltpu.VMEM((rows, width), f32),
            pltpu.VMEM((2, count, 3, planes + 2, k + 2 * PAD, width), f32),
            bonds,
            bonds,
            pltpu.VMEM((count, planes, k, width), f32),
            bonds,
            bonds,
            bonds,
            bonds,
            pltpu.VMEM((2, count, 3, planes, k, width), f32),
            pltpu.VMEM((count, 8, width), f32),
            pltpu.VMEM((n - 1, count, 8, width), f32),
            pltpu.VMEM((3, 8, width), f32),
            pltpu.VMEM((3, 8, width), f32),
            pltpu.VMEM((2, 3, planes, rows, width), f32),
            dma((5,)),
            dma((2,)),
            dma((HALVES, count, 2)),
            dma((HALVES, count, 2)),
            dma((n - 1,)),
            dma((n - 1,)),
            dma((2,)),
            dma((2,)),
            dma((planes, 2)),
            dma((planes, 2)),
        ],
        compiler_params=pltpu.CompilerParams(
            collective_id=0, has_side_effects=True, vmem_limit_bytes=48 * 1024 * 1024
        ),
    )(spin, coup, beta, order, level, height, angle, bits)


def solution(mesh):
    n, m = mesh.shape["gz"], mesh.shape["temp"]
    return jax.shard_map(
        functools.partial(on_device, n, m),
        mesh=mesh,
        in_specs=(
            P(("group", "temp"), None, "gz", None, None),
            P(None, ("group", "gz"), None, None),
            P(("group", "temp")),
            P(("group", "temp")),
            P(("group", "temp"), "gz", None, None),
            P(("group", "temp"), "gz", None, None),
            P(("group", "temp"), "gz", None, None),
            P(("group", "temp")),
        ),
        out_specs=(P(("group", "temp"), None, "gz", None, None), P(("group", "temp"))),
        check_vma=False,
    )
```

```python
import functools
import math

import jax
import jax.numpy as jnp
from jax import lax
from jax.experimental import pallas as pl
from jax.experimental.pallas import tpu as pltpu
from jax.sharding import PartitionSpec as P

OR_SWEEPS = 2
HALVES = 2 * OR_SWEEPS + 2
PAD = 8
MESH = pl.DeviceIdType.MESH
SIN_TERMS = [(-1.0) ** i / math.factorial(2 * i + 1) for i in range(8)]
COS_TERMS = [(-1.0) ** i / math.factorial(2 * i) for i in range(9)]


def horner(terms, value):
    total = jnp.full_like(value, terms[-1])
    for term in terms[-2::-1]:
        total = total * value + term
    return total


def cos_sin(angle):
    half = 0.5 * angle
    square = half * half
    sine = half * horner(SIN_TERMS, square)
    cosine = horner(COS_TERMS, square)
    return 1.0 - 2.0 * sine * sine, 2.0 * sine * cosine


def dot3(a, b):
    return a[0] * b[0] + a[1] * b[1] + a[2] * b[2]


def reflect(current, pulled):
    factor = 2.0 * dot3(current, pulled) / jnp.maximum(dot3(pulled, pulled), 0.01)
    return [factor * p - s for p, s in zip(pulled, current)]


def heat_bath(pulled, beta, level, trial):
    strength = jnp.sqrt(jnp.maximum(dot3(pulled, pulled), 0.01))
    inverse = 1.0 / strength
    axis = [p * inverse for p in pulled]
    reach = beta * strength
    shrink = -jnp.tanh(reach) * (jnp.exp(-2.0 * reach) + 1.0)
    cosine = 1.0 + jnp.log1p(level * shrink) / reach
    along = dot3(trial, axis)
    tangent = [t - along * a for t, a in zip(trial, axis)]
    scale = jnp.sqrt(jnp.maximum(1.0 - cosine * cosine, 0.0)) * (
        1.0 / jnp.sqrt(jnp.maximum(dot3(tangent, tangent), 0.0001))
    )
    return [cosine * a + scale * t for a, t in zip(axis, tangent)]


def kernel(
    dims,
    spin_hbm,
    coup_hbm,
    beta_ref,
    order_ref,
    level_hbm,
    height_hbm,
    angle_hbm,
    bits_ref,
    out_ref,
    eout_ref,
    spin_in,
    coup_in,
    level_in,
    height_in,
    angle_in,
    below_bond,
    sp,
    xo,
    xr,
    yi,
    yo,
    zu,
    zd,
    lv,
    ut,
    eacc,
    ebuf,
    tsend,
    trecv,
    rbuf,
    in_sem,
    bond_sem,
    hsend,
    hrecv,
    esend,
    erecv,
    tssem,
    trsem,
    xsend,
    xrecv,
):
    count, planes, rows, width, n, m = dims
    k = rows // 2
    chunk = 32 if k % 32 == 0 else 8
    g = lax.axis_index("gz")
    t = lax.axis_index("temp")
    up, down = lax.rem(g + 1, n), lax.rem(g + n - 1, n)
    has_below, has_above = t > 0, t < m - 1

    loads = [
        pltpu.make_async_copy(src, dst, in_sem.at[i])
        for i, (src, dst) in enumerate(
            (
                (spin_hbm.at[:, :, pl.ds(0, 1)], spin_in.at[:, :, pl.ds(0, 1)]),
                (
                    spin_hbm.at[:, :, pl.ds(planes - 1, 1)],
                    spin_in.at[:, :, pl.ds(planes - 1, 1)],
                ),
                (coup_hbm, coup_in),
                (
                    spin_hbm.at[:, :, pl.ds(1, planes - 2)],
                    spin_in.at[:, :, pl.ds(1, planes - 2)],
                ),
                (level_hbm, level_in),
                (height_hbm, height_in),
                (angle_hbm, angle_in),
            )
        )
    ]
    for load in loads:
        load.start()

    barrier = pltpu.get_barrier_semaphore()
    for d in range(1, n):
        pl.semaphore_signal(
            barrier, inc=1, device_id={"gz": lax.rem(g + d, n)}, device_id_type=MESH
        )

    @pl.when(has_below)
    def _():
        pl.semaphore_signal(barrier, inc=1, device_id={"temp": t - 1}, device_id_type=MESH)

    @pl.when(has_above)
    def _():
        pl.semaphore_signal(barrier, inc=1, device_id={"temp": t + 1}, device_id_type=MESH)

    pl.semaphore_wait(barrier, n - 1 + has_below.astype(jnp.int32) + has_above.astype(jnp.int32))

    def parity(r, z, size):
        lane = lax.broadcasted_iota(jnp.int32, (size, width), 1)
        return ((lane + (g * planes + z + order_ref[r])) & 1) != 0

    def halves(ref, index, start, size):
        even = ref[index + (pl.ds(2 * start, size, stride=2), slice(None))]
        odd = ref[index + (pl.ds(2 * start + 1, size, stride=2), slice(None))]
        return even, odd

    def put_spin(c, r, d, z, start, value):
        size = value.shape[0]
        sp[c, r, d, z + 1, pl.ds(PAD + start, size), :] = value
        if start == 0:
            sp[c, r, d, z + 1, pl.ds(PAD + k, 1), :] = value[0:1]
        if start + size == k:
            sp[c, r, d, z + 1, pl.ds(PAD - 1, 1), :] = value[size - 1 : size]

    def pack_spin(r, z):
        e = parity(r, z, k)
        for d in range(3):
            even, odd = halves(spin_in, (r, d, z), 0, k)
            put_spin(0, r, d, z, 0, jnp.where(e, odd, even))
            put_spin(1, r, d, z, 0, jnp.where(e, even, odd))

    def halo(x, r, side):
        c = 1 - x % 2
        source, target = (1, planes + 1) if side == 0 else (planes, 0)
        return pltpu.make_async_remote_copy(
            src_ref=sp.at[c, r, :, source, pl.ds(PAD, k), :],
            dst_ref=sp.at[c, r, :, target, pl.ds(PAD, k), :],
            send_sem=hsend.at[x, r, side],
            recv_sem=hrecv.at[x, r, side],
            device_id={"gz": down if side == 0 else up},
            device_id_type=MESH,
        )

    def edges(r, action):
        def step(i, carry):
            action(r, i * (planes - 1))
            return carry

        lax.fori_loop(0, 2, step, 0)

    def inner(action):
        def step(i, carry):
            action(i // (planes - 2), 1 + i % (planes - 2))
            return carry

        if planes > 2:
            lax.fori_loop(0, count * (planes - 2), step, 0)

    loads[0].wait()
    loads[1].wait()
    for r in range(count):
        edges(r, pack_spin)
        for side in (0, 1):
            halo(0, r, side).start()
    loads[2].wait()
    bond = pltpu.make_async_remote_copy(
        src_ref=coup_in.at[2, planes - 1],
        dst_ref=below_bond,
        send_sem=bond_sem.at[0],
        recv_sem=bond_sem.at[1],
        device_id={"gz": up},
        device_id_type=MESH,
    )
    bond.start()
    loads[3].wait()
    inner(pack_spin)

    def pack_bonds(i, carry):
        r, z = i // planes, i % planes
        e = parity(r, z, k)
        even, odd = halves(coup_in, (0, z), 0, k)
        first, second = jnp.where(e, odd, even), jnp.where(e, even, odd)
        xo[0, r, z] = first
        xo[1, r, z] = second
        xr[0, r, z] = pltpu.roll(second, 1, 1)
        xr[1, r, z] = pltpu.roll(first, 1, 1)
        even, odd = halves(coup_in, (1, z), 0, k)
        before = pltpu.roll(odd, 1, 0)
        yi[r, z] = even
        yo[0, r, z] = jnp.where(e, odd, before)
        yo[1, r, z] = jnp.where(e, before, odd)
        even, odd = halves(coup_in, (2, z), 0, k)
        zu[0, r, z] = jnp.where(e, odd, even)
        zu[1, r, z] = jnp.where(e, even, odd)
        return carry

    def pack_lower(i, carry):
        r, z = i // (planes - 1), 1 + i % (planes - 1)
        e = parity(r, z, k)
        even, odd = halves(coup_in, (2, z - 1), 0, k)
        zd[0, r, z] = jnp.where(e, odd, even)
        zd[1, r, z] = jnp.where(e, even, odd)
        return carry

    lax.fori_loop(0, count * planes, pack_bonds, 0)
    lax.fori_loop(0, count * (planes - 1), pack_lower, 0)
    bond.wait()
    for r in range(count):
        e = parity(r, 0, k)
        even, odd = halves(below_bond, (), 0, k)
        zd[0, r, 0] = jnp.where(e, odd, even)
        zd[1, r, 0] = jnp.where(e, even, odd)

    def pull(c, r, z, start):
        o = 1 - c
        part = pl.ds(start, chunk)
        e = parity(r, z, chunk)
        bx, br, by = xo[c, r, z, part, :], xr[c, r, z, part, :], yi[r, z, part, :]
        bo, bu, bd = yo[c, r, z, part, :], zu[c, r, z, part, :], zd[c, r, z, part, :]
        pulled = []
        for d in range(3):
            mid = sp[o, r, d, z + 1, pl.ds(PAD + start, chunk), :]
            nxt = sp[o, r, d, z + 1, pl.ds(PAD + start + 1, chunk), :]
            prv = sp[o, r, d, z + 1, pl.ds(PAD + start - 1, chunk), :]
            outer = jnp.where(e, nxt, prv) if c == 0 else jnp.where(e, prv, nxt)
            total = bx * pltpu.roll(mid, width - 1, 1) + br * pltpu.roll(mid, 1, 1)
            total = total + by * mid + bo * outer
            total = total + bu * sp[o, r, d, z + 2, pl.ds(PAD + start, chunk), :]
            total = total + bd * sp[o, r, d, z, pl.ds(PAD + start, chunk), :]
            pulled.append(total)
        return pulled

    def relax(c, r, z):
        for start in range(0, k, chunk):
            pulled = pull(c, r, z, start)
            current = [sp[c, r, d, z + 1, pl.ds(PAD + start, chunk), :] for d in range(3)]
            for d, value in enumerate(reflect(current, pulled)):
                put_spin(c, r, d, z, start, value)

    def heat(c, r, z):
        for start in range(0, k, chunk):
            part = pl.ds(start, chunk)
            pulled = pull(c, r, z, start)
            trial = [ut[c, r, d, z, part, :] for d in range(3)]
            renewed = heat_bath(pulled, beta_ref[r], lv[c, r, z, part, :], trial)
            for d, value in enumerate(renewed):
                put_spin(c, r, d, z, start, value)
            if c == 1:
                terms = dot3(renewed, pulled)
                eacc[r] = eacc[r] + sum(terms[j : j + 8] for j in range(0, chunk, 8))

    def pack_heat(r):
        def step(z, carry):
            for start in range(0, k, chunk):
                part = pl.ds(start, chunk)
                e = parity(r, z, chunk)
                even, odd = halves(level_in, (r, z), start, chunk)
                lv[0, r, z, part, :] = jnp.where(e, odd, even)
                lv[1, r, z, part, :] = jnp.where(e, even, odd)
                angles = halves(angle_in, (r, z), start, chunk)
                heights = halves(height_in, (r, z), start, chunk)
                trials = []
                for angle, height in zip(angles, heights):
                    side = jnp.sqrt(jnp.maximum(1.0 - height * height, 0.0))
                    cosine, sine = cos_sin(angle)
                    trials.append((side * cosine, side * sine, height))
                for d in range(3):
                    ut[0, r, d, z, part, :] = jnp.where(e, trials[1][d], trials[0][d])
                    ut[1, r, d, z, part, :] = jnp.where(e, trials[0][d], trials[1][d])
            return carry

        lax.fori_loop(0, planes, step, 0)

    def take_halo(x, r):
        for side in (0, 1):
            halo(x, r, side).wait_recv()
            if x >= 1:
                halo(x - 1, r, side).wait_send()

    eacc[...] = jnp.zeros_like(eacc)
    for x in range(HALVES - 1):
        c = x % 2
        work = functools.partial(relax if x < 2 * OR_SWEEPS else heat, c)
        for r in range(count):
            take_halo(x, r)
            edges(r, work)
            for side in (0, 1):
                halo(x + 1, r, side).start()
        inner(work)
        if x == 0:
            for load in loads[4:]:
                load.wait()
        for r in range(count):
            if r % (2 * OR_SWEEPS) == x:
                pack_heat(r)

    def flag(j, size):
        return jnp.full((size, width), bits_ref[j], jnp.int32) != 0

    def unpack(z):
        for r in range(0, count, 2):
            taking = flag(r, k)
            masks = [parity(r + j, z, k) for j in (0, 1)]
            for d in range(3):
                both = []
                for j in (0, 1):
                    first = sp[0, r + j, d, z + 1, pl.ds(PAD, k), :]
                    second = sp[1, r + j, d, z + 1, pl.ds(PAD, k), :]
                    both.append(
                        (jnp.where(masks[j], second, first), jnp.where(masks[j], first, second))
                    )
                for row in (0, 1):
                    low, top = both[0][row], both[1][row]
                    place = pl.ds(row, k, stride=2)
                    out_ref[r, d, z, place, :] = jnp.where(taking, top, low)
                    out_ref[r + 1, d, z, place, :] = jnp.where(taking, low, top)

    def ship(z, side):
        return pltpu.make_async_remote_copy(
            src_ref=out_ref.at[count - 1 if side == 0 else 0, :, z],
            dst_ref=rbuf.at[side, :, z],
            send_sem=xsend.at[z, side],
            recv_sem=xrecv.at[z, side],
            device_id={"temp": t + 1 if side == 0 else t - 1},
            device_id_type=MESH,
        )

    def finish(plane_list):
        for z in plane_list:
            unpack(z)

            @pl.when(has_above)
            def _():
                ship(z, 0).start()

            @pl.when(has_below)
            def _():
                ship(z, 1).start()

    x = HALVES - 1
    work = functools.partial(heat, 1)
    inner(work)
    middle = list(range(1, planes - 1))
    outside = [0, planes - 1]
    finish(middle)
    for r in range(count):
        take_halo(x, r)
        edges(r, work)
    swaps = []
    for d in range(1, n):
        swaps.append(
            pltpu.make_async_remote_copy(
                src_ref=eacc,
                dst_ref=ebuf.at[d - 1],
                send_sem=esend.at[d - 1],
                recv_sem=erecv.at[d - 1],
                device_id={"gz": lax.rem(g + d, n)},
                device_id_type=MESH,
            )
        )
    for swap in swaps:
        swap.start()
    finish(outside)

    for swap in swaps:
        swap.wait()
    sites = float(width * rows * planes * n)
    energy = []
    for r in range(count):
        total = eacc[r]
        for d in range(n - 1):
            total = total + ebuf[d, r]
        summed = jnp.sum(jnp.sum(total, axis=0, keepdims=True), axis=1, keepdims=True)
        energy.append(jnp.broadcast_to(-summed / sites, (8, width)))
    for r in range(0, count, 2):
        taking = flag(r, 8)
        low, top = energy[r], energy[r + 1]
        energy[r], energy[r + 1] = jnp.where(taking, top, low), jnp.where(taking, low, top)
    tsend[0] = energy[count - 1]
    tsend[1] = jnp.full((8, width), bits_ref[count - 1], jnp.int32).astype(jnp.float32)
    tsend[2] = energy[0]

    def tell(side):
        part = pl.ds(0, 2) if side == 0 else pl.ds(2, 1)
        return pltpu.make_async_remote_copy(
            src_ref=tsend.at[part],
            dst_ref=trecv.at[part],
            send_sem=tssem.at[side],
            recv_sem=trsem.at[side],
            device_id={"temp": t + 1 if side == 0 else t - 1},
            device_id_type=MESH,
        )

    @pl.when(has_above)
    def _():
        tell(0).start()

    @pl.when(has_below)
    def _():
        tell(1).start()

    for r in range(1, count - 1, 2):
        taking = flag(r, 8)
        low, top = energy[r], energy[r + 1]
        energy[r], energy[r + 1] = jnp.where(taking, top, low), jnp.where(taking, low, top)
        wide = flag(r, rows)

        def exchange(i, carry):
            d, z = i // planes, i % planes
            a, b = out_ref[r, d, z], out_ref[r + 1, d, z]
            out_ref[r, d, z] = jnp.where(wide, b, a)
            out_ref[r + 1, d, z] = jnp.where(wide, a, b)
            return carry

        lax.fori_loop(0, 3 * planes, exchange, 0)

    for r in range(count):
        eout_ref[r] = jnp.max(energy[r])

    for r in range(count):
        for side in (0, 1):
            halo(x, r, side).wait_send()

    @pl.when(has_above)
    def _():
        tell(0).wait_send()
        tell(1).wait_recv()
        wide = flag(count - 1, rows)
        eout_ref[count - 1] = jnp.max(
            jnp.where(flag(count - 1, 8), trecv[2], energy[count - 1])
        )
        for z in middle + outside:
            ship(z, 0).wait_send()
            ship(z, 1).wait_recv()
            for d in range(3):
                out_ref[count - 1, d, z] = jnp.where(wide, rbuf[1, d, z], out_ref[count - 1, d, z])

    @pl.when(has_below)
    def _():
        tell(1).wait_send()
        tell(0).wait_recv()
        eout_ref[0] = jnp.max(jnp.where(trecv[1] > 0.5, trecv[0], energy[0]))
        wide = jnp.broadcast_to(trecv[1][0:1], (rows, width)) > 0.5
        for z in middle + outside:
            ship(z, 1).wait_send()
            ship(z, 0).wait_recv()
            for d in range(3):
                out_ref[0, d, z] = jnp.where(wide, rbuf[0, d, z], out_ref[0, d, z])


def on_device(n, m, spin, coup, beta, order, level, height, angle, bits):
    count, _, planes, rows, width = spin.shape
    k = rows // 2
    f32 = jnp.float32
    hbm = pl.BlockSpec(memory_space=pltpu.HBM)
    smem = pl.BlockSpec(memory_space=pltpu.SMEM)
    dma = pltpu.SemaphoreType.DMA
    bonds = pltpu.VMEM((2, count, planes, k, width), f32)
    return pl.pallas_call(
        functools.partial(kernel, (count, planes, rows, width, n, m)),
        out_shape=(
            jax.ShapeDtypeStruct(spin.shape, f32),
            jax.ShapeDtypeStruct((count,), f32),
        ),
        in_specs=[hbm, hbm, smem, smem, hbm, hbm, hbm, smem],
        out_specs=(pl.BlockSpec(memory_space=pltpu.VMEM), smem),
        scratch_shapes=[
            pltpu.VMEM(spin.shape, f32),
            pltpu.VMEM(coup.shape, f32),
            pltpu.VMEM(level.shape, f32),
            pltpu.VMEM(level.shape, f32),
            pltpu.VMEM(level.shape, f32),
            pltpu.VMEM((rows, width), f32),
            pltpu.VMEM((2, count, 3, planes + 2, k + 2 * PAD, width), f32),
            bonds,
            bonds,
            pltpu.VMEM((count, planes, k, width), f32),
            bonds,
            bonds,
            bonds,
            bonds,
            pltpu.VMEM((2, count, 3, planes, k, width), f32),
            pltpu.VMEM((count, 8, width), f32),
            pltpu.VMEM((n - 1, count, 8, width), f32),
            pltpu.VMEM((3, 8, width), f32),
            pltpu.VMEM((3, 8, width), f32),
            pltpu.VMEM((2, 3, planes, rows, width), f32),
            dma((7,)),
            dma((2,)),
            dma((HALVES, count, 2)),
            dma((HALVES, count, 2)),
            dma((n - 1,)),
            dma((n - 1,)),
            dma((2,)),
            dma((2,)),
            dma((planes, 2)),
            dma((planes, 2)),
        ],
        compiler_params=pltpu.CompilerParams(
            collective_id=0, has_side_effects=True, vmem_limit_bytes=60 * 1024 * 1024
        ),
    )(spin, coup, beta, order, level, height, angle, bits)


def solution(mesh):
    n, m = mesh.shape["gz"], mesh.shape["temp"]
    return jax.shard_map(
        functools.partial(on_device, n, m),
        mesh=mesh,
        in_specs=(
            P(("group", "temp"), None, "gz", None, None),
            P(None, ("group", "gz"), None, None),
            P(("group", "temp")),
            P(("group", "temp")),
            P(("group", "temp"), "gz", None, None),
            P(("group", "temp"), "gz", None, None),
            P(("group", "temp"), "gz", None, None),
            P(("group", "temp")),
        ),
        out_specs=(P(("group", "temp"), None, "gz", None, None), P(("group", "temp"))),
        check_vma=False,
    )
```

```python
import functools
import math

import jax
import jax.numpy as jnp
from jax import lax
from jax.experimental import pallas as pl
from jax.experimental.pallas import tpu as pltpu
from jax.sharding import PartitionSpec as P

OR_SWEEPS = 2
HALVES = 2 * OR_SWEEPS + 2
PAD = 8
MESH = pl.DeviceIdType.MESH
SIN_TERMS = [(-1.0) ** i / math.factorial(2 * i + 1) for i in range(8)]
COS_TERMS = [(-1.0) ** i / math.factorial(2 * i) for i in range(9)]


def horner(terms, value):
    total = jnp.full_like(value, terms[-1])
    for term in terms[-2::-1]:
        total = total * value + term
    return total


def cos_sin(angle):
    half = 0.5 * angle
    square = half * half
    sine = half * horner(SIN_TERMS, square)
    cosine = horner(COS_TERMS, square)
    return 1.0 - 2.0 * sine * sine, 2.0 * sine * cosine


def dot3(a, b):
    return a[0] * b[0] + a[1] * b[1] + a[2] * b[2]


def reflect(current, pulled):
    factor = 2.0 * dot3(current, pulled) / jnp.maximum(dot3(pulled, pulled), 0.01)
    return [factor * p - s for p, s in zip(pulled, current)]


def heat_bath(pulled, beta, level, trial):
    strength = jnp.sqrt(jnp.maximum(dot3(pulled, pulled), 0.01))
    inverse = 1.0 / strength
    axis = [p * inverse for p in pulled]
    reach = beta * strength
    shrink = -jnp.tanh(reach) * (jnp.exp(-2.0 * reach) + 1.0)
    cosine = 1.0 + jnp.log1p(level * shrink) / reach
    along = dot3(trial, axis)
    tangent = [t - along * a for t, a in zip(trial, axis)]
    scale = jnp.sqrt(jnp.maximum(1.0 - cosine * cosine, 0.0)) * (
        1.0 / jnp.sqrt(jnp.maximum(dot3(tangent, tangent), 0.0001))
    )
    return [cosine * a + scale * t for a, t in zip(axis, tangent)]


def kernel(
    dims,
    spin_hbm,
    coup_hbm,
    beta_ref,
    order_ref,
    level_hbm,
    height_hbm,
    angle_hbm,
    bits_ref,
    out_ref,
    eout_ref,
    spin_in,
    coup_in,
    level_in,
    height_in,
    angle_in,
    lifted,
    sp,
    xo,
    xr,
    yi,
    yo,
    zu,
    zd,
    lv,
    ut,
    eacc,
    ebuf,
    tsend,
    trecv,
    rbuf,
    in_sem,
    hsend,
    hrecv,
    esend,
    erecv,
    tssem,
    trsem,
    xsend,
    xrecv,
):
    count, planes, rows, width, n, m = dims
    k = rows // 2
    chunk = 32 if k % 32 == 0 else 8
    g = lax.axis_index("gz")
    t = lax.axis_index("temp")
    up, down = lax.rem(g + 1, n), lax.rem(g + n - 1, n)
    has_below, has_above = t > 0, t < m - 1

    loads = [
        pltpu.make_async_copy(src, dst, in_sem.at[i])
        for i, (src, dst) in enumerate(
            (
                (spin_hbm.at[:, :, pl.ds(0, 1)], spin_in.at[:, :, pl.ds(0, 1)]),
                (
                    spin_hbm.at[:, :, pl.ds(planes - 1, 1)],
                    spin_in.at[:, :, pl.ds(planes - 1, 1)],
                ),
                (coup_hbm.at[2, planes - 1], coup_in.at[2, planes - 1]),
                (coup_hbm.at[pl.ds(0, 2)], coup_in.at[pl.ds(0, 2)]),
                (
                    coup_hbm.at[2, pl.ds(0, planes - 1)],
                    coup_in.at[2, pl.ds(0, planes - 1)],
                ),
                (
                    spin_hbm.at[:, :, pl.ds(1, planes - 2)],
                    spin_in.at[:, :, pl.ds(1, planes - 2)],
                ),
                (level_hbm, level_in),
                (height_hbm, height_in),
                (angle_hbm, angle_in),
            )
        )
    ]
    for load in loads:
        load.start()

    barrier = pltpu.get_barrier_semaphore()
    for d in range(1, n):
        pl.semaphore_signal(
            barrier, inc=1, device_id={"gz": lax.rem(g + d, n)}, device_id_type=MESH
        )

    @pl.when(has_below)
    def _():
        pl.semaphore_signal(barrier, inc=1, device_id={"temp": t - 1}, device_id_type=MESH)

    @pl.when(has_above)
    def _():
        pl.semaphore_signal(barrier, inc=1, device_id={"temp": t + 1}, device_id_type=MESH)

    pl.semaphore_wait(barrier, n - 1 + has_below.astype(jnp.int32) + has_above.astype(jnp.int32))

    def parity(r, z, size):
        lane = lax.broadcasted_iota(jnp.int32, (size, width), 1)
        return ((lane + (g * planes + z + order_ref[r])) & 1) != 0

    def halves(ref, index, start, size):
        even = ref[index + (pl.ds(2 * start, size, stride=2), slice(None))]
        odd = ref[index + (pl.ds(2 * start + 1, size, stride=2), slice(None))]
        return even, odd

    def put_spin(c, r, d, z, start, value):
        size = value.shape[0]
        sp[c, r, d, z + 1, pl.ds(PAD + start, size), :] = value
        if start == 0:
            sp[c, r, d, z + 1, pl.ds(PAD + k, 1), :] = value[0:1]
        if start + size == k:
            sp[c, r, d, z + 1, pl.ds(PAD - 1, 1), :] = value[size - 1 : size]

    def pack_spin(r, z):
        e = parity(r, z, k)
        for d in range(3):
            even, odd = halves(spin_in, (r, d, z), 0, k)
            put_spin(0, r, d, z, 0, jnp.where(e, odd, even))
            put_spin(1, r, d, z, 0, jnp.where(e, even, odd))

    def halo(x, r, side):
        c = 1 - x % 2
        plain = sp.at[c, r, :, 1, pl.ds(PAD, k), :]
        return pltpu.make_async_remote_copy(
            src_ref=plain if side == 0 else lifted.at[c, r],
            dst_ref=sp.at[c, r, :, planes + 1 if side == 0 else 0, pl.ds(PAD, k), :],
            send_sem=hsend.at[x, r, side],
            recv_sem=hrecv.at[x, r, side],
            device_id={"gz": down if side == 0 else up},
            device_id_type=MESH,
        )

    def lift(c, r, d, start, value):
        part = pl.ds(start, value.shape[0])
        lifted[c, r, d, part, :] = zu[c, r, planes - 1, part, :] * value

    def inner(action):
        def step(i, carry):
            action(i // (planes - 2), 1 + i % (planes - 2))
            return carry

        if planes > 2:
            lax.fori_loop(0, count * (planes - 2), step, 0)

    for load in loads[:3]:
        load.wait()
    for r in range(count):
        pack_spin(r, 0)
        halo(0, r, 0).start()
        e = parity(r, planes - 1, k)
        even, odd = halves(coup_in, (2, planes - 1), 0, k)
        zu[0, r, planes - 1] = jnp.where(e, odd, even)
        zu[1, r, planes - 1] = jnp.where(e, even, odd)
        pack_spin(r, planes - 1)
        for d in range(3):
            lift(1, r, d, 0, sp[1, r, d, planes, pl.ds(PAD, k), :])
        halo(0, r, 1).start()
    for load in loads[3:6]:
        load.wait()
    inner(pack_spin)

    def pack_bonds(i, carry):
        r, z = i // planes, i % planes
        e = parity(r, z, k)
        even, odd = halves(coup_in, (0, z), 0, k)
        first, second = jnp.where(e, odd, even), jnp.where(e, even, odd)
        xo[0, r, z] = first
        xo[1, r, z] = second
        xr[0, r, z] = pltpu.roll(second, 1, 1)
        xr[1, r, z] = pltpu.roll(first, 1, 1)
        even, odd = halves(coup_in, (1, z), 0, k)
        before = pltpu.roll(odd, 1, 0)
        yi[r, z] = even
        yo[0, r, z] = jnp.where(e, odd, before)
        yo[1, r, z] = jnp.where(e, before, odd)
        return carry

    def pack_lower(i, carry):
        r, z = i // (planes - 1), 1 + i % (planes - 1)
        e = parity(r, z, k)
        even, odd = halves(coup_in, (2, z - 1), 0, k)
        zd[0, r, z] = jnp.where(e, odd, even)
        zd[1, r, z] = jnp.where(e, even, odd)
        zu[0, r, z - 1] = jnp.where(e, even, odd)
        zu[1, r, z - 1] = jnp.where(e, odd, even)
        return carry

    lax.fori_loop(0, count * planes, pack_bonds, 0)
    lax.fori_loop(0, count * (planes - 1), pack_lower, 0)
    for r in range(count):
        for c in (0, 1):
            zd[c, r, 0] = jnp.ones((k, width), jnp.float32)

    def pull(c, r, z, start):
        o = 1 - c
        part = pl.ds(start, chunk)
        e = parity(r, z, chunk)
        bx, br, by = xo[c, r, z, part, :], xr[c, r, z, part, :], yi[r, z, part, :]
        bo, bu, bd = yo[c, r, z, part, :], zu[c, r, z, part, :], zd[c, r, z, part, :]
        pulled = []
        for d in range(3):
            mid = sp[o, r, d, z + 1, pl.ds(PAD + start, chunk), :]
            nxt = sp[o, r, d, z + 1, pl.ds(PAD + start + 1, chunk), :]
            prv = sp[o, r, d, z + 1, pl.ds(PAD + start - 1, chunk), :]
            outer = jnp.where(e, nxt, prv) if c == 0 else jnp.where(e, prv, nxt)
            total = bx * pltpu.roll(mid, width - 1, 1) + br * pltpu.roll(mid, 1, 1)
            total = total + by * mid + bo * outer
            total = total + bu * sp[o, r, d, z + 2, pl.ds(PAD + start, chunk), :]
            total = total + bd * sp[o, r, d, z, pl.ds(PAD + start, chunk), :]
            pulled.append(total)
        return pulled

    def relax(c, r, z, lifting=False):
        for start in range(0, k, chunk):
            pulled = pull(c, r, z, start)
            current = [sp[c, r, d, z + 1, pl.ds(PAD + start, chunk), :] for d in range(3)]
            for d, value in enumerate(reflect(current, pulled)):
                put_spin(c, r, d, z, start, value)
                if lifting:
                    lift(c, r, d, start, value)

    def heat(c, r, z, lifting=False):
        for start in range(0, k, chunk):
            part = pl.ds(start, chunk)
            pulled = pull(c, r, z, start)
            trial = [ut[c, r, d, z, part, :] for d in range(3)]
            renewed = heat_bath(pulled, beta_ref[r], lv[c, r, z, part, :], trial)
            for d, value in enumerate(renewed):
                put_spin(c, r, d, z, start, value)
                if lifting:
                    lift(c, r, d, start, value)
            if c == 1:
                terms = dot3(renewed, pulled)
                eacc[r] = eacc[r] + sum(terms[j : j + 8] for j in range(0, chunk, 8))

    def pack_heat(r):
        def step(z, carry):
            for start in range(0, k, chunk):
                part = pl.ds(start, chunk)
                e = parity(r, z, chunk)
                even, odd = halves(level_in, (r, z), start, chunk)
                lv[0, r, z, part, :] = jnp.where(e, odd, even)
                lv[1, r, z, part, :] = jnp.where(e, even, odd)
                angles = halves(angle_in, (r, z), start, chunk)
                heights = halves(height_in, (r, z), start, chunk)
                trials = []
                for angle, height in zip(angles, heights):
                    side = jnp.sqrt(jnp.maximum(1.0 - height * height, 0.0))
                    cosine, sine = cos_sin(angle)
                    trials.append((side * cosine, side * sine, height))
                for d in range(3):
                    ut[0, r, d, z, part, :] = jnp.where(e, trials[1][d], trials[0][d])
                    ut[1, r, d, z, part, :] = jnp.where(e, trials[0][d], trials[1][d])
            return carry

        lax.fori_loop(0, planes, step, 0)

    def take_halo(x, r, side):
        halo(x, r, 1 - side).wait_recv()
        if x >= 1:
            halo(x - 1, r, side).wait_send()

    eacc[...] = jnp.zeros_like(eacc)
    for x in range(HALVES - 1):
        c = x % 2
        work = functools.partial(relax if x < 2 * OR_SWEEPS else heat, c)
        for r in range(count):
            for side, z in ((0, 0), (1, planes - 1)):
                take_halo(x, r, side)
                work(r, z, lifting=side == 1)
                halo(x + 1, r, side).start()
        inner(work)
        if x == 0:
            for load in loads[6:]:
                load.wait()
        for r in range(count):
            if r % (2 * OR_SWEEPS) == x:
                pack_heat(r)

    def flag(j, size):
        return jnp.full((size, width), bits_ref[j], jnp.int32) != 0

    def unpack(z):
        for r in range(0, count, 2):
            taking = flag(r, k)
            masks = [parity(r + j, z, k) for j in (0, 1)]
            for d in range(3):
                both = []
                for j in (0, 1):
                    first = sp[0, r + j, d, z + 1, pl.ds(PAD, k), :]
                    second = sp[1, r + j, d, z + 1, pl.ds(PAD, k), :]
                    both.append(
                        (jnp.where(masks[j], second, first), jnp.where(masks[j], first, second))
                    )
                for row in (0, 1):
                    low, top = both[0][row], both[1][row]
                    place = pl.ds(row, k, stride=2)
                    out_ref[r, d, z, place, :] = jnp.where(taking, top, low)
                    out_ref[r + 1, d, z, place, :] = jnp.where(taking, low, top)

    def ship(z, side):
        return pltpu.make_async_remote_copy(
            src_ref=out_ref.at[count - 1 if side == 0 else 0, :, z],
            dst_ref=rbuf.at[side, :, z],
            send_sem=xsend.at[z, side],
            recv_sem=xrecv.at[z, side],
            device_id={"temp": t + 1 if side == 0 else t - 1},
            device_id_type=MESH,
        )

    def finish(plane_list):
        for z in plane_list:
            unpack(z)

            @pl.when(has_above)
            def _():
                ship(z, 0).start()

            @pl.when(has_below)
            def _():
                ship(z, 1).start()

    x = HALVES - 1
    work = functools.partial(heat, 1)
    inner(work)
    middle = list(range(1, planes - 1))
    outside = [0, planes - 1]
    finish(middle)
    for r in range(count):
        for side, z in ((0, 0), (1, planes - 1)):
            take_halo(x, r, side)
            work(r, z)
    swaps = []
    for d in range(1, n):
        swaps.append(
            pltpu.make_async_remote_copy(
                src_ref=eacc,
                dst_ref=ebuf.at[d - 1],
                send_sem=esend.at[d - 1],
                recv_sem=erecv.at[d - 1],
                device_id={"gz": lax.rem(g + d, n)},
                device_id_type=MESH,
            )
        )
    for swap in swaps:
        swap.start()
    finish(outside)

    for swap in swaps:
        swap.wait()
    sites = float(width * rows * planes * n)
    energy = []
    for r in range(count):
        total = eacc[r]
        for d in range(n - 1):
            total = total + ebuf[d, r]
        summed = jnp.sum(jnp.sum(total, axis=0, keepdims=True), axis=1, keepdims=True)
        energy.append(jnp.broadcast_to(-summed / sites, (8, width)))
    for r in range(0, count, 2):
        taking = flag(r, 8)
        low, top = energy[r], energy[r + 1]
        energy[r], energy[r + 1] = jnp.where(taking, top, low), jnp.where(taking, low, top)
    tsend[0] = energy[count - 1]
    tsend[1] = jnp.full((8, width), bits_ref[count - 1], jnp.int32).astype(jnp.float32)
    tsend[2] = energy[0]

    def tell(side):
        part = pl.ds(0, 2) if side == 0 else pl.ds(2, 1)
        return pltpu.make_async_remote_copy(
            src_ref=tsend.at[part],
            dst_ref=trecv.at[part],
            send_sem=tssem.at[side],
            recv_sem=trsem.at[side],
            device_id={"temp": t + 1 if side == 0 else t - 1},
            device_id_type=MESH,
        )

    @pl.when(has_above)
    def _():
        tell(0).start()

    @pl.when(has_below)
    def _():
        tell(1).start()

    for r in range(1, count - 1, 2):
        taking = flag(r, 8)
        low, top = energy[r], energy[r + 1]
        energy[r], energy[r + 1] = jnp.where(taking, top, low), jnp.where(taking, low, top)
        wide = flag(r, rows)

        def exchange(i, carry):
            d, z = i // planes, i % planes
            a, b = out_ref[r, d, z], out_ref[r + 1, d, z]
            out_ref[r, d, z] = jnp.where(wide, b, a)
            out_ref[r + 1, d, z] = jnp.where(wide, a, b)
            return carry

        lax.fori_loop(0, 3 * planes, exchange, 0)

    for r in range(count):
        eout_ref[r] = jnp.max(energy[r])

    for r in range(count):
        for side in (0, 1):
            halo(x, r, side).wait_send()

    @pl.when(has_above)
    def _():
        tell(0).wait_send()
        tell(1).wait_recv()
        wide = flag(count - 1, rows)
        eout_ref[count - 1] = jnp.max(
            jnp.where(flag(count - 1, 8), trecv[2], energy[count - 1])
        )
        for z in middle + outside:
            ship(z, 0).wait_send()
            ship(z, 1).wait_recv()
            for d in range(3):
                out_ref[count - 1, d, z] = jnp.where(wide, rbuf[1, d, z], out_ref[count - 1, d, z])

    @pl.when(has_below)
    def _():
        tell(1).wait_send()
        tell(0).wait_recv()
        eout_ref[0] = jnp.max(jnp.where(trecv[1] > 0.5, trecv[0], energy[0]))
        wide = jnp.broadcast_to(trecv[1][0:1], (rows, width)) > 0.5
        for z in middle + outside:
            ship(z, 1).wait_send()
            ship(z, 0).wait_recv()
            for d in range(3):
                out_ref[0, d, z] = jnp.where(wide, rbuf[0, d, z], out_ref[0, d, z])


def on_device(n, m, spin, coup, beta, order, level, height, angle, bits):
    count, _, planes, rows, width = spin.shape
    k = rows // 2
    f32 = jnp.float32
    hbm = pl.BlockSpec(memory_space=pltpu.HBM)
    smem = pl.BlockSpec(memory_space=pltpu.SMEM)
    dma = pltpu.SemaphoreType.DMA
    bonds = pltpu.VMEM((2, count, planes, k, width), f32)
    return pl.pallas_call(
        functools.partial(kernel, (count, planes, rows, width, n, m)),
        out_shape=(
            jax.ShapeDtypeStruct(spin.shape, f32),
            jax.ShapeDtypeStruct((count,), f32),
        ),
        in_specs=[hbm, hbm, smem, smem, hbm, hbm, hbm, smem],
        out_specs=(pl.BlockSpec(memory_space=pltpu.VMEM), smem),
        scratch_shapes=[
            pltpu.VMEM(spin.shape, f32),
            pltpu.VMEM(coup.shape, f32),
            pltpu.VMEM(level.shape, f32),
            pltpu.VMEM(level.shape, f32),
            pltpu.VMEM(level.shape, f32),
            pltpu.VMEM((2, count, 3, k, width), f32),
            pltpu.VMEM((2, count, 3, planes + 2, k + 2 * PAD, width), f32),
            bonds,
            bonds,
            pltpu.VMEM((count, planes, k, width), f32),
            bonds,
            bonds,
            bonds,
            bonds,
            pltpu.VMEM((2, count, 3, planes, k, width), f32),
            pltpu.VMEM((count, 8, width), f32),
            pltpu.VMEM((n - 1, count, 8, width), f32),
            pltpu.VMEM((3, 8, width), f32),
            pltpu.VMEM((3, 8, width), f32),
            pltpu.VMEM((2, 3, planes, rows, width), f32),
            dma((9,)),
            dma((HALVES, count, 2)),
            dma((HALVES, count, 2)),
            dma((n - 1,)),
            dma((n - 1,)),
            dma((2,)),
            dma((2,)),
            dma((planes, 2)),
            dma((planes, 2)),
        ],
        compiler_params=pltpu.CompilerParams(
            collective_id=0, has_side_effects=True, vmem_limit_bytes=60 * 1024 * 1024
        ),
    )(spin, coup, beta, order, level, height, angle, bits)


def solution(mesh):
    n, m = mesh.shape["gz"], mesh.shape["temp"]
    return jax.shard_map(
        functools.partial(on_device, n, m),
        mesh=mesh,
        in_specs=(
            P(("group", "temp"), None, "gz", None, None),
            P(None, ("group", "gz"), None, None),
            P(("group", "temp")),
            P(("group", "temp")),
            P(("group", "temp"), "gz", None, None),
            P(("group", "temp"), "gz", None, None),
            P(("group", "temp"), "gz", None, None),
            P(("group", "temp")),
        ),
        out_specs=(P(("group", "temp"), None, "gz", None, None), P(("group", "temp"))),
        check_vma=False,
    )
```

```python
import functools
import math

import jax
import jax.numpy as jnp
from jax import lax
from jax.experimental import pallas as pl
from jax.experimental.pallas import tpu as pltpu
from jax.sharding import PartitionSpec as P

OR_SWEEPS = 2
HALVES = 2 * OR_SWEEPS + 2
PAD = 8
MESH = pl.DeviceIdType.MESH
SIN_TERMS = [(-1.0) ** i / math.factorial(2 * i + 1) for i in range(8)]
COS_TERMS = [(-1.0) ** i / math.factorial(2 * i) for i in range(9)]


def horner(terms, value):
    total = jnp.full_like(value, terms[-1])
    for term in terms[-2::-1]:
        total = total * value + term
    return total


def cos_sin(angle):
    half = 0.5 * angle
    square = half * half
    sine = half * horner(SIN_TERMS, square)
    cosine = horner(COS_TERMS, square)
    return 1.0 - 2.0 * sine * sine, 2.0 * sine * cosine


def dot3(a, b):
    return a[0] * b[0] + a[1] * b[1] + a[2] * b[2]


def reflect(current, pulled):
    factor = 2.0 * dot3(current, pulled) / jnp.maximum(dot3(pulled, pulled), 0.01)
    return [factor * p - s for p, s in zip(pulled, current)]


def heat_bath(pulled, beta, level, trial):
    strength = jnp.sqrt(jnp.maximum(dot3(pulled, pulled), 0.01))
    inverse = 1.0 / strength
    axis = [p * inverse for p in pulled]
    reach = beta * strength
    shrink = -jnp.tanh(reach) * (jnp.exp(-2.0 * reach) + 1.0)
    cosine = 1.0 + jnp.log1p(level * shrink) / reach
    along = dot3(trial, axis)
    tangent = [t - along * a for t, a in zip(trial, axis)]
    scale = jnp.sqrt(jnp.maximum(1.0 - cosine * cosine, 0.0)) * (
        1.0 / jnp.sqrt(jnp.maximum(dot3(tangent, tangent), 0.0001))
    )
    return [cosine * a + scale * t for a, t in zip(axis, tangent)]


def kernel(
    dims,
    spin_hbm,
    coup_hbm,
    beta_ref,
    order_ref,
    level_hbm,
    height_hbm,
    angle_hbm,
    bits_ref,
    out_ref,
    eout_ref,
    spin_in,
    coup_in,
    level_in,
    height_in,
    angle_in,
    lifted,
    sp,
    xo,
    xr,
    yi,
    yo,
    zu,
    zd,
    lv,
    ut,
    eacc,
    ebuf,
    tsend,
    trecv,
    rbuf,
    in_sem,
    hsend,
    hrecv,
    esend,
    erecv,
    tssem,
    trsem,
    xsend,
    xrecv,
):
    count, planes, rows, width, n, m = dims
    k = rows // 2
    chunk = 32 if k % 32 == 0 else 8
    g = lax.axis_index("gz")
    t = lax.axis_index("temp")
    up, down = lax.rem(g + 1, n), lax.rem(g + n - 1, n)
    has_below, has_above = t > 0, t < m - 1

    loads = [
        pltpu.make_async_copy(src, dst, in_sem.at[i])
        for i, (src, dst) in enumerate(
            (
                (spin_hbm.at[:, :, pl.ds(0, 1)], spin_in.at[:, :, pl.ds(0, 1)]),
                (
                    spin_hbm.at[:, :, pl.ds(planes - 1, 1)],
                    spin_in.at[:, :, pl.ds(planes - 1, 1)],
                ),
                (coup_hbm.at[2, planes - 1], coup_in.at[2, planes - 1]),
                (coup_hbm.at[pl.ds(0, 2)], coup_in.at[pl.ds(0, 2)]),
                (
                    coup_hbm.at[2, pl.ds(0, planes - 1)],
                    coup_in.at[2, pl.ds(0, planes - 1)],
                ),
                (
                    spin_hbm.at[:, :, pl.ds(1, planes - 2)],
                    spin_in.at[:, :, pl.ds(1, planes - 2)],
                ),
                (level_hbm, level_in),
                (height_hbm, height_in),
                (angle_hbm, angle_in),
            )
        )
    ]
    for load in loads:
        load.start()

    barrier = pltpu.get_barrier_semaphore()
    for d in range(1, n):
        pl.semaphore_signal(
            barrier, inc=1, device_id={"gz": lax.rem(g + d, n)}, device_id_type=MESH
        )

    @pl.when(has_below)
    def _():
        pl.semaphore_signal(barrier, inc=1, device_id={"temp": t - 1}, device_id_type=MESH)

    @pl.when(has_above)
    def _():
        pl.semaphore_signal(barrier, inc=1, device_id={"temp": t + 1}, device_id_type=MESH)

    pl.semaphore_wait(barrier, n - 1 + has_below.astype(jnp.int32) + has_above.astype(jnp.int32))

    def parity(r, z, size):
        lane = lax.broadcasted_iota(jnp.int32, (size, width), 1)
        return ((lane + (g * planes + z + order_ref[r])) & 1) != 0

    def halves(ref, index, start, size):
        even = ref[index + (pl.ds(2 * start, size, stride=2), slice(None))]
        odd = ref[index + (pl.ds(2 * start + 1, size, stride=2), slice(None))]
        return even, odd

    def put_spin(c, r, d, z, start, value):
        size = value.shape[0]
        sp[c, r, d, z + 1, pl.ds(PAD + start, size), :] = value
        if start == 0:
            sp[c, r, d, z + 1, pl.ds(PAD + k, 1), :] = value[0:1]
        if start + size == k:
            sp[c, r, d, z + 1, pl.ds(PAD - 1, 1), :] = value[size - 1 : size]

    def pack_spin(r, z):
        e = parity(r, z, k)
        for d in range(3):
            even, odd = halves(spin_in, (r, d, z), 0, k)
            put_spin(0, r, d, z, 0, jnp.where(e, odd, even))
            put_spin(1, r, d, z, 0, jnp.where(e, even, odd))

    def halo(x, r, side):
        c = 1 - x % 2
        plain = sp.at[c, r, :, 1, pl.ds(PAD, k), :]
        return pltpu.make_async_remote_copy(
            src_ref=plain if side == 0 else lifted.at[c, r],
            dst_ref=sp.at[c, r, :, planes + 1 if side == 0 else 0, pl.ds(PAD, k), :],
            send_sem=hsend.at[x, r, side],
            recv_sem=hrecv.at[x, r, side],
            device_id={"gz": down if side == 0 else up},
            device_id_type=MESH,
        )

    def lift(c, r, d, start, value):
        part = pl.ds(start, value.shape[0])
        lifted[c, r, d, part, :] = zu[c, r, planes - 1, part, :] * value

    def inner(action):
        def step(i, carry):
            action(i // (planes - 2), 1 + i % (planes - 2))
            return carry

        if planes > 2:
            lax.fori_loop(0, count * (planes - 2), step, 0)

    for load in loads[:3]:
        load.wait()
    for r in range(count):
        pack_spin(r, 0)
        halo(0, r, 0).start()
        e = parity(r, planes - 1, k)
        even, odd = halves(coup_in, (2, planes - 1), 0, k)
        zu[0, r, planes - 1] = jnp.where(e, odd, even)
        zu[1, r, planes - 1] = jnp.where(e, even, odd)
        pack_spin(r, planes - 1)
        for d in range(3):
            lift(1, r, d, 0, sp[1, r, d, planes, pl.ds(PAD, k), :])
        halo(0, r, 1).start()
    for load in loads[3:6]:
        load.wait()
    inner(pack_spin)

    def pack_bonds(i, carry):
        r, z = i // planes, i % planes
        e = parity(r, z, k)
        even, odd = halves(coup_in, (0, z), 0, k)
        first, second = jnp.where(e, odd, even), jnp.where(e, even, odd)
        xo[0, r, z] = first
        xo[1, r, z] = second
        xr[0, r, z] = pltpu.roll(second, 1, 1)
        xr[1, r, z] = pltpu.roll(first, 1, 1)
        even, odd = halves(coup_in, (1, z), 0, k)
        before = pltpu.roll(odd, 1, 0)
        yi[r, z] = even
        yo[0, r, z] = jnp.where(e, odd, before)
        yo[1, r, z] = jnp.where(e, before, odd)
        return carry

    def pack_lower(i, carry):
        r, z = i // (planes - 1), 1 + i % (planes - 1)
        e = parity(r, z, k)
        even, odd = halves(coup_in, (2, z - 1), 0, k)
        zd[0, r, z] = jnp.where(e, odd, even)
        zd[1, r, z] = jnp.where(e, even, odd)
        zu[0, r, z - 1] = jnp.where(e, even, odd)
        zu[1, r, z - 1] = jnp.where(e, odd, even)
        return carry

    lax.fori_loop(0, count * planes, pack_bonds, 0)
    lax.fori_loop(0, count * (planes - 1), pack_lower, 0)
    for r in range(count):
        for c in (0, 1):
            zd[c, r, 0] = jnp.ones((k, width), jnp.float32)

    def pull(c, r, z, start):
        o = 1 - c
        part = pl.ds(start, chunk)
        e = parity(r, z, chunk)
        bx, br, by = xo[c, r, z, part, :], xr[c, r, z, part, :], yi[r, z, part, :]
        bo, bu, bd = yo[c, r, z, part, :], zu[c, r, z, part, :], zd[c, r, z, part, :]
        pulled = []
        for d in range(3):
            mid = sp[o, r, d, z + 1, pl.ds(PAD + start, chunk), :]
            nxt = sp[o, r, d, z + 1, pl.ds(PAD + start + 1, chunk), :]
            prv = sp[o, r, d, z + 1, pl.ds(PAD + start - 1, chunk), :]
            outer = jnp.where(e, nxt, prv) if c == 0 else jnp.where(e, prv, nxt)
            total = bx * pltpu.roll(mid, width - 1, 1) + br * pltpu.roll(mid, 1, 1)
            total = total + by * mid + bo * outer
            total = total + bu * sp[o, r, d, z + 2, pl.ds(PAD + start, chunk), :]
            total = total + bd * sp[o, r, d, z, pl.ds(PAD + start, chunk), :]
            pulled.append(total)
        return pulled

    def relax(c, r, z, lifting=False):
        for start in range(0, k, chunk):
            pulled = pull(c, r, z, start)
            current = [sp[c, r, d, z + 1, pl.ds(PAD + start, chunk), :] for d in range(3)]
            for d, value in enumerate(reflect(current, pulled)):
                put_spin(c, r, d, z, start, value)
                if lifting:
                    lift(c, r, d, start, value)

    def heat(c, r, z, lifting=False):
        for start in range(0, k, chunk):
            part = pl.ds(start, chunk)
            pulled = pull(c, r, z, start)
            trial = [ut[c, r, d, z, part, :] for d in range(3)]
            renewed = heat_bath(pulled, beta_ref[r], lv[c, r, z, part, :], trial)
            for d, value in enumerate(renewed):
                put_spin(c, r, d, z, start, value)
                if lifting:
                    lift(c, r, d, start, value)
            if c == 1:
                terms = dot3(renewed, pulled)
                eacc[r] = eacc[r] + sum(terms[j : j + 8] for j in range(0, chunk, 8))

    def pack_heat(r):
        def step(z, carry):
            for start in range(0, k, chunk):
                part = pl.ds(start, chunk)
                e = parity(r, z, chunk)
                even, odd = halves(level_in, (r, z), start, chunk)
                lv[0, r, z, part, :] = jnp.where(e, odd, even)
                lv[1, r, z, part, :] = jnp.where(e, even, odd)
                angles = halves(angle_in, (r, z), start, chunk)
                heights = halves(height_in, (r, z), start, chunk)
                trials = []
                for angle, height in zip(angles, heights):
                    side = jnp.sqrt(jnp.maximum(1.0 - height * height, 0.0))
                    cosine, sine = cos_sin(angle)
                    trials.append((side * cosine, side * sine, height))
                for d in range(3):
                    ut[0, r, d, z, part, :] = jnp.where(e, trials[1][d], trials[0][d])
                    ut[1, r, d, z, part, :] = jnp.where(e, trials[0][d], trials[1][d])
            return carry

        lax.fori_loop(0, planes, step, 0)

    def take_halo(x, r, side):
        halo(x, r, 1 - side).wait_recv()
        if x >= 1:
            halo(x - 1, r, side).wait_send()

    eacc[...] = jnp.zeros_like(eacc)
    for x in range(HALVES - 1):
        c = x % 2
        work = functools.partial(relax if x < 2 * OR_SWEEPS else heat, c)
        for r in range(count):
            for side, z in ((0, 0), (1, planes - 1)):
                take_halo(x, r, side)
                work(r, z, lifting=side == 1)
                halo(x + 1, r, side).start()
        inner(work)
        if x == 0:
            for load in loads[6:]:
                load.wait()
        for r in range(count):
            if r % (2 * OR_SWEEPS) == x:
                pack_heat(r)

    def flag(j, size):
        return jnp.full((size, width), bits_ref[j], jnp.int32) != 0

    def unpack(z):
        for r in range(0, count, 2):
            taking = flag(r, k)
            masks = [parity(r + j, z, k) for j in (0, 1)]
            for d in range(3):
                both = []
                for j in (0, 1):
                    first = sp[0, r + j, d, z + 1, pl.ds(PAD, k), :]
                    second = sp[1, r + j, d, z + 1, pl.ds(PAD, k), :]
                    both.append(
                        (jnp.where(masks[j], second, first), jnp.where(masks[j], first, second))
                    )
                for row in (0, 1):
                    low, top = both[0][row], both[1][row]
                    place = pl.ds(row, k, stride=2)
                    out_ref[r, d, z, place, :] = jnp.where(taking, top, low)
                    out_ref[r + 1, d, z, place, :] = jnp.where(taking, low, top)

    def ship(z, side):
        return pltpu.make_async_remote_copy(
            src_ref=out_ref.at[count - 1 if side == 0 else 0, :, z],
            dst_ref=rbuf.at[side, :, z],
            send_sem=xsend.at[z, side],
            recv_sem=xrecv.at[z, side],
            device_id={"temp": t + 1 if side == 0 else t - 1},
            device_id_type=MESH,
        )

    def finish(plane_list):
        for z in plane_list:
            unpack(z)

            @pl.when(has_above)
            def _():
                ship(z, 0).start()

            @pl.when(has_below)
            def _():
                ship(z, 1).start()

    x = HALVES - 1
    work = functools.partial(heat, 1)
    inner(work)
    middle = list(range(1, planes - 1))
    outside = [0, planes - 1]
    finish(middle)
    for side, z in ((0, 0), (1, planes - 1)):
        for r in range(count):
            take_halo(x, r, side)
            work(r, z)
        if side == 0:
            finish([z])
    swaps = []
    for d in range(1, n):
        swaps.append(
            pltpu.make_async_remote_copy(
                src_ref=eacc,
                dst_ref=ebuf.at[d - 1],
                send_sem=esend.at[d - 1],
                recv_sem=erecv.at[d - 1],
                device_id={"gz": lax.rem(g + d, n)},
                device_id_type=MESH,
            )
        )
    for swap in swaps:
        swap.start()
    finish([planes - 1])

    for swap in swaps:
        swap.wait()
    sites = float(width * rows * planes * n)
    energy = []
    for r in range(count):
        total = eacc[r]
        for d in range(n - 1):
            total = total + ebuf[d, r]
        summed = jnp.sum(jnp.sum(total, axis=0, keepdims=True), axis=1, keepdims=True)
        energy.append(jnp.broadcast_to(-summed / sites, (8, width)))
    for r in range(0, count, 2):
        taking = flag(r, 8)
        low, top = energy[r], energy[r + 1]
        energy[r], energy[r + 1] = jnp.where(taking, top, low), jnp.where(taking, low, top)
    tsend[0] = energy[count - 1]
    tsend[1] = jnp.full((8, width), bits_ref[count - 1], jnp.int32).astype(jnp.float32)
    tsend[2] = energy[0]

    def tell(side):
        part = pl.ds(0, 2) if side == 0 else pl.ds(2, 1)
        return pltpu.make_async_remote_copy(
            src_ref=tsend.at[part],
            dst_ref=trecv.at[part],
            send_sem=tssem.at[side],
            recv_sem=trsem.at[side],
            device_id={"temp": t + 1 if side == 0 else t - 1},
            device_id_type=MESH,
        )

    @pl.when(has_above)
    def _():
        tell(0).start()

    @pl.when(has_below)
    def _():
        tell(1).start()

    for r in range(1, count - 1, 2):
        taking = flag(r, 8)
        low, top = energy[r], energy[r + 1]
        energy[r], energy[r + 1] = jnp.where(taking, top, low), jnp.where(taking, low, top)
        wide = flag(r, rows)

        def exchange(i, carry):
            d, z = i // planes, i % planes
            a, b = out_ref[r, d, z], out_ref[r + 1, d, z]
            out_ref[r, d, z] = jnp.where(wide, b, a)
            out_ref[r + 1, d, z] = jnp.where(wide, a, b)
            return carry

        lax.fori_loop(0, 3 * planes, exchange, 0)

    for r in range(count):
        eout_ref[r] = jnp.max(energy[r])

    for r in range(count):
        for side in (0, 1):
            halo(x, r, side).wait_send()

    @pl.when(has_above)
    def _():
        tell(0).wait_send()
        tell(1).wait_recv()
        wide = flag(count - 1, rows)
        eout_ref[count - 1] = jnp.max(
            jnp.where(flag(count - 1, 8), trecv[2], energy[count - 1])
        )
        for z in middle + outside:
            ship(z, 0).wait_send()
            ship(z, 1).wait_recv()
            for d in range(3):
                out_ref[count - 1, d, z] = jnp.where(wide, rbuf[1, d, z], out_ref[count - 1, d, z])

    @pl.when(has_below)
    def _():
        tell(1).wait_send()
        tell(0).wait_recv()
        eout_ref[0] = jnp.max(jnp.where(trecv[1] > 0.5, trecv[0], energy[0]))
        wide = jnp.broadcast_to(trecv[1][0:1], (rows, width)) > 0.5
        for z in middle + outside:
            ship(z, 1).wait_send()
            ship(z, 0).wait_recv()
            for d in range(3):
                out_ref[0, d, z] = jnp.where(wide, rbuf[0, d, z], out_ref[0, d, z])


def on_device(n, m, spin, coup, beta, order, level, height, angle, bits):
    count, _, planes, rows, width = spin.shape
    k = rows // 2
    f32 = jnp.float32
    hbm = pl.BlockSpec(memory_space=pltpu.HBM)
    smem = pl.BlockSpec(memory_space=pltpu.SMEM)
    dma = pltpu.SemaphoreType.DMA
    bonds = pltpu.VMEM((2, count, planes, k, width), f32)
    return pl.pallas_call(
        functools.partial(kernel, (count, planes, rows, width, n, m)),
        out_shape=(
            jax.ShapeDtypeStruct(spin.shape, f32),
            jax.ShapeDtypeStruct((count,), f32),
        ),
        in_specs=[hbm, hbm, smem, smem, hbm, hbm, hbm, smem],
        out_specs=(pl.BlockSpec(memory_space=pltpu.VMEM), smem),
        scratch_shapes=[
            pltpu.VMEM(spin.shape, f32),
            pltpu.VMEM(coup.shape, f32),
            pltpu.VMEM(level.shape, f32),
            pltpu.VMEM(level.shape, f32),
            pltpu.VMEM(level.shape, f32),
            pltpu.VMEM((2, count, 3, k, width), f32),
            pltpu.VMEM((2, count, 3, planes + 2, k + 2 * PAD, width), f32),
            bonds,
            bonds,
            pltpu.VMEM((count, planes, k, width), f32),
            bonds,
            bonds,
            bonds,
            bonds,
            pltpu.VMEM((2, count, 3, planes, k, width), f32),
            pltpu.VMEM((count, 8, width), f32),
            pltpu.VMEM((n - 1, count, 8, width), f32),
            pltpu.VMEM((3, 8, width), f32),
            pltpu.VMEM((3, 8, width), f32),
            pltpu.VMEM((2, 3, planes, rows, width), f32),
            dma((9,)),
            dma((HALVES, count, 2)),
            dma((HALVES, count, 2)),
            dma((n - 1,)),
            dma((n - 1,)),
            dma((2,)),
            dma((2,)),
            dma((planes, 2)),
            dma((planes, 2)),
        ],
        compiler_params=pltpu.CompilerParams(
            collective_id=0, has_side_effects=True, vmem_limit_bytes=60 * 1024 * 1024
        ),
    )(spin, coup, beta, order, level, height, angle, bits)


def solution(mesh):
    n, m = mesh.shape["gz"], mesh.shape["temp"]
    return jax.shard_map(
        functools.partial(on_device, n, m),
        mesh=mesh,
        in_specs=(
            P(("group", "temp"), None, "gz", None, None),
            P(None, ("group", "gz"), None, None),
            P(("group", "temp")),
            P(("group", "temp")),
            P(("group", "temp"), "gz", None, None),
            P(("group", "temp"), "gz", None, None),
            P(("group", "temp"), "gz", None, None),
            P(("group", "temp")),
        ),
        out_specs=(P(("group", "temp"), None, "gz", None, None), P(("group", "temp"))),
        check_vma=False,
    )
```
